256 devices in a mesh: row: 16 (over y, z_hi, core), col: 16 (over z_lo, x).
Axes of the slice: x: 4, y: 4, z: 8 (z_hi: 2, z_lo: 4; z = z_hi * 4 + z_lo), core: 2. Of those that a mesh axis runs over, the one named last changes fastest.
Arguments:
- fluid_data: float32 [51, 32768], P(None, ('row', 'col')), as said below
- center_data: float32 [51, 16384], P(None, ('col', 'row')), as said below
- poly_coef: float32 [48, 4], replicated, may hold values from -3 to 3
Outputs:
- fluid_motion: float32 [48, 32768], P(None, ('row', 'col'))
- center_load: float32 [48, 16384], P(None, ('col', 'row'))
The draws below stay inside these ranges and needn't reach their ends.
Inputs may be any that keep to these rules, and one draw needn't show every extreme that they name: Rows 0 to 2 of fluid_data lie in [0, 1]; rows 3 and on are forces. Rows 0 and 1 of center_data lie in [0, 1] and row 2 lies in [-0.5, -0.02], so every center is at least 0.02 below every vertex; rows 3 and on are coefficients.
All inputs are finite; a program needn't handle non-finite values.
Results may differ from the reference program's by a relative error of at most 0.0003.
Values sent between devices are 32-bit elements; how exact they have to be, the bound alone decides.
A program may use at most 64 MiB of HBM per device.

```python
import math
import jax
import jax.numpy as jnp
from jax import lax

WAVES = 64
COLS = 48
FLUID = 32768
CENTERS = 16384


def draw_fluid_data(key, part):
    first, second = jax.random.split(jax.random.fold_in(key, 11))
    places = jax.random.uniform(first, (3, FLUID), jnp.float32)
    spread = 2.0 * math.pi * WAVES * math.sqrt(0.8 / FLUID)
    values = jax.random.normal(second, (COLS, FLUID), jnp.float32) * spread
    return jnp.concatenate([places, values], axis=0)


def draw_center_data(key, part):
    first, second, third = jax.random.split(jax.random.fold_in(key, 23), 3)
    plane = jax.random.uniform(first, (2, CENTERS), jnp.float32)
    depth = jax.random.uniform(second, (1, CENTERS), jnp.float32)
    spread = 2.0 * math.pi * WAVES * math.sqrt(0.8 / CENTERS)
    height = -0.02 - 0.48 * depth
    values = jax.random.normal(third, (COLS, CENTERS), jnp.float32) * spread
    return jnp.concatenate([plane, height, values], axis=0)


def noise(key, dims, scale, limit, kind=jnp.bfloat16):
    entries = scale * jax.random.normal(key, dims, jnp.float32)
    return jnp.clip(entries, min=-limit, max=limit).astype(kind)


def setup_inputs(seed: int = 0) -> dict:
    streams_of = jax.random.split(jax.random.key(seed), 4)
    fluid_data = draw_fluid_data(jax.random.fold_in(streams_of[3], 71), 0)
    center_data = draw_center_data(jax.random.fold_in(streams_of[3], 71), 0)
    poly_coef = noise(streams_of[2], (COLS, 4), 0.5, 3.0, jnp.float32)
    return dict(fluid_data=fluid_data, center_data=center_data, poly_coef=poly_coef)


def kernel_block(center_pos, fluid_pos):
    dx = center_pos[0][:, None] - fluid_pos[0][None, :]
    dy = center_pos[1][:, None] - fluid_pos[1][None, :]
    dz = center_pos[2][:, None] - fluid_pos[2][None, :]
    sq = dx * dx + dy * dy + dz * dz
    phase = 2.0 * math.pi * WAVES * jnp.sqrt(sq)
    return jnp.sin(phase) / phase

def reference(fluid_data, center_data, poly_coef):
    total = center_data.shape[1]
    width = fluid_data.shape[1]
    block = math.gcd(total, 256)
    count = total // block
    fluid_pos = fluid_data[:3]
    forces = fluid_data[3:]
    pieces = center_data.reshape(center_data.shape[0], count, block).transpose(1, 0, 2)

    def step(motion, piece):
        tile = kernel_block(piece[:3], fluid_pos)
        motion = motion + jnp.dot(piece[3:], tile, precision=lax.Precision.HIGHEST, preferred_element_type=jnp.float32)
        back = lax.dot_general(forces, tile, (((1,), (1,)), ((), ())), precision=lax.Precision.HIGHEST, preferred_element_type=jnp.float32)
        return (motion, back)
    start = jnp.zeros((forces.shape[0], width), jnp.float32)
    motion, backs = lax.scan(step, start, pieces)
    loads = backs.transpose(1, 0, 2).reshape(forces.shape[0], total)
    affine = poly_coef[:, 0:1] + jnp.dot(poly_coef[:, 1:], fluid_pos, precision=lax.Precision.HIGHEST, preferred_element_type=jnp.float32)
    return (motion + affine, loads)
```

```python
import functools

import jax
import jax.numpy as jnp
from jax import lax
from jax.experimental import pallas as pl
from jax.experimental.pallas import tpu as pltpu
from jax.sharding import PartitionSpec as P

WAVES = 64
MESH = pl.DeviceIdType.MESH
TOP = 12.404427306735432
MID = 0.6418441597071612
LOW = 0.16126480593510223


def paired(me, m, n):
    other, bit = 0, 1
    while bit < n:
        other = other + (((me // bit) % 2 + (m // bit) % 2) % 2) * bit
        bit *= 2
    return other


def dot(a, b, dims):
    return lax.dot_general(a, b, (dims, ((), ())), preferred_element_type=jnp.float32)


def split(x):
    high = x.astype(jnp.bfloat16)
    low = (x - high.astype(jnp.float32)).astype(jnp.bfloat16)
    return high, low


def body(rows, cols, side, fluid, center, poly, motion, loads, *scratch):
    fl, ce, pv, cp, chl, fhl, kh, kl, mo_out, mo_in, ld_out, ld_in, pre = scratch[:13]
    own, fs, fr, cs, cr, ms, mr, ls, lr, ps, pr = scratch[13:]
    S, T = cols // side, rows * side
    half = T // 2
    row, col = lax.axis_index("row"), lax.axis_index("col")
    side = S // 2
    my_s = ((row // 2) % 2) * side + col // side
    my_t = (row % 2) * half + (row // 4) * 4 + col % 4
    nvals = pv.shape[1]
    wf, wc = fluid.shape[1], center.shape[1]
    lanes = 128 if wf % 128 == 0 else wf
    step_rows = 32 if wc % 32 == 0 else wc

    def along_s(m):
        i = paired(my_s, m, S)
        return {"row": (row // 4) * 4 + (i // 4) * 2 + row % 2, "col": (i % 4) * 4 + col % 4}

    def along_t(m):
        i = paired(my_t, m, T)
        return {
            "row": ((i % 16) // 4) * 4 + ((row // 2) % 2) * 2 + i // 16,
            "col": (col // 4) * 4 + i % 4,
        }

    def copy(src, dst, send, recv, where):
        return pltpu.make_async_remote_copy(
            src_ref=src, dst_ref=dst, send_sem=send, recv_sem=recv, device_id=where, device_id_type=MESH
        )

    def send_fluid(m):
        return copy(fl.at[0], fl.at[m], fs.at[m], fr.at[m], along_s(m))

    def send_center(p):
        return copy(ce.at[0], ce.at[p], cs.at[p], cr.at[p], along_t(half if p == 1 else p - 1))

    def hand_on(p):
        q = p + half - 1
        return copy(ce.at[p], ce.at[q], cs.at[q], cr.at[q], along_t(half))

    def send_motion(m):
        return copy(mo_out.at[m], mo_in.at[m], ms.at[m], mr.at[m], along_s(m))

    def send_pre(p):
        j = p - half
        return copy(ld_out.at[p], pre.at[j], ps.at[j], pr.at[j], along_t(half))

    def send_loads(j):
        return copy(ld_out.at[j + 1], ld_in.at[j], ls.at[j], lr.at[j], along_t(j))

    def send_other():
        return copy(ld_out.at[1], ld_in.at[0], ls.at[0], lr.at[0], along_t(half))

    local = [
        pltpu.make_async_copy(center, ce.at[0], own.at[0]),
        pltpu.make_async_copy(fluid, fl.at[0], own.at[1]),
        pltpu.make_async_copy(poly, pv, own.at[2]),
    ]
    for c in local:
        c.start()
    barrier = pltpu.get_barrier_semaphore()
    for p in range(1, half + 1):
        pl.semaphore_signal(barrier, inc=1, device_id=along_t(p), device_id_type=MESH)
    for m in range(1, S):
        pl.semaphore_signal(barrier, inc=1, device_id=along_s(m), device_id_type=MESH)
    for c in local:
        c.wait()
    order_s = [1] + list(range(S - 1, 1, -1))
    pl.semaphore_wait(barrier, S - 1 + half)
    for p in range(1, half + 1):
        send_center(p).start()
    for m in order_s:
        send_fluid(m).start()

    def ready_center(r):
        places = jnp.transpose(ce[r, 0:8, :] * float(WAVES))
        for a in range(3):
            cp[r, a] = jnp.broadcast_to(places[:, a : a + 1], (wc, lanes))
        high, low = split(ce[r, 3:, :] * TOP)
        chl[r, 0:nvals] = high
        chl[r, nvals:] = low
        ld_out[r] = jnp.zeros((nvals, wc), jnp.float32)

    def ready_fluid(m):
        high, low = split(fl[m, 3:, :] * TOP)
        fhl[m, 0:nvals] = high
        fhl[m, nvals:] = low
        mo_out[m] = jnp.zeros((nvals, wf), jnp.float32)

    def values(m, r, slot):
        for h in range(wf // lanes):
            part = pl.ds(h * lanes, lanes)
            fx, fy, fz = (fl[m, a : a + 1, part] * float(WAVES) for a in range(3))
            for j in range(0, wc, step_rows):
                at = pl.ds(j, step_rows)
                dx, dy, dz = cp[r, 0, at, :] - fx, cp[r, 1, at, :] - fy, cp[r, 2, at, :] - fz
                sq = dx * dx + dy * dy + dz * dz
                inv = lax.rsqrt(sq)
                turns = sq * inv
                f = turns - jnp.round(turns)
                size = jnp.abs(f)
                rest = 0.5 - size
                q = size * rest
                value = (f * rest * inv) * ((q + MID) * q + LOW)
                high, low = split(value)
                kh[slot, at, part] = high
                kl[slot, at, part] = low

    def sums(m, r, slot):
        k_high, k_low = kh[slot], kl[slot]
        across = ((1,), (0,))
        wide = dot(chl[r], k_high, across)
        mo_out[m] += wide[:nvals] + wide[nvals:] + dot(chl[r, 0:nvals], k_low, across)
        back = ((1,), (1,))
        wide = dot(fhl[m], k_high, back)
        ld_out[r] += wide[:nvals] + wide[nvals:] + dot(fhl[m, 0:nvals], k_low, back)

    def pair(before, one, two):
        sums(*before, 1)
        values(*one, 0)
        sums(*one, 0)
        values(*two, 1)
        return two

    kh[1] = jnp.zeros((wc, wf), jnp.bfloat16)
    kl[1] = jnp.zeros((wc, wf), jnp.bfloat16)
    ready_fluid(0)
    before = (0, 0)

    for k in range(half):
        for p in (2 * k, 2 * k + 1):
            if 2 <= p <= half:
                send_center(p).wait_recv()
                hand_on(p).start()
            elif p == 1:
                send_center(p).wait_recv()
            elif p > half:
                hand_on(p - half + 1).wait_recv()
            ready_center(p)
        if k == 0:
            send_fluid(order_s[0]).wait_recv()
            ready_fluid(order_s[0])
        m = order_s[0]
        before = pair(before, (m, 2 * k), (m, 2 * k + 1))

    def middle(s, _):
        m = S - s
        send_fluid(m).wait_recv()
        ready_fluid(m)
        last_m = (m + 1) % S + (m + 1) // S

        pair((last_m, T - 1), (m, 0), (m, 1))
        send_motion(last_m).start()

        def inner(k, _):
            pair((m, 2 * k - 1), (m, 2 * k), (m, 2 * k + 1))
            return 0

        lax.fori_loop(1, half, inner, 0)
        return 0

    lax.fori_loop(1, S - 2, middle, 0)

    far = order_s[-1]
    prior = order_s[-2]
    send_fluid(far).wait_recv()
    ready_fluid(far)
    pair((prior, T - 1), (far, T - 1), (0, T - 1))
    send_motion(prior).start()

    def mixed(k, _):
        r = T - 1 - k
        pair((0, r + 1), (far, r), (0, r))
        send_pre(r + 1).start()
        return 0

    lax.fori_loop(1, half, mixed, 0)

    def finish(j):
        send_pre(half + j).wait_recv()
        ld_out[j + 1] += pre[j]
        send_loads(j).start()

    pair((0, half), (far, half - 1), (far, half - 2))
    finish(half - 1)

    def far_rest(k, _):
        r = half - 1 - 2 * k
        pair((far, r + 1), (far, r), (far, r - 1))
        return 0

    lax.fori_loop(1, half // 2, far_rest, 0)
    pair((far, 0), (0, half - 1), (0, half - 2))
    send_motion(far).start()
    finish(half - 2)

    def own_rest(k, _):
        r = half - 1 - 2 * k
        pair((0, r + 1), (0, r), (0, r - 1))
        finish(r)

        @pl.when(r > 1)
        def _():
            finish(r - 1)

        return 0

    lax.fori_loop(1, half // 2, own_rest, 0)
    send_other().start()
    sums(0, 0, 1)

    total = mo_out[0]
    affine = jnp.transpose(pv[...])
    for a in range(3):
        total = total + affine[:, a + 1 : a + 2] * fl[0, a : a + 1, :]
    total = total + affine[:, 0:1]
    for m in order_s:
        send_motion(m).wait_recv()
        total = total + mo_in[m]
    motion[...] = total
    total = ld_out[0]
    for j in range(half - 1, 0, -1):
        send_loads(j).wait_recv()
        total = total + ld_in[j]
    send_other().wait_recv()
    loads[...] = total + ld_in[0]
    for m in order_s:
        send_fluid(m).wait_send()
        send_motion(m).wait_send()
    for p in range(1, half + 1):
        send_center(p).wait_send()
    for p in range(2, half + 1):
        hand_on(p).wait_send()
        send_pre(p + half - 1).wait_send()
        send_loads(p - 1).wait_send()
    send_other().wait_send()


def per_device(rows, cols, side, fluid_data, center_data, poly_coef):
    f32, bf16 = jnp.float32, jnp.bfloat16
    S, T = cols // side, rows * side
    height, wf = fluid_data.shape
    wc = center_data.shape[1]
    n = height - 3
    lanes = 128 if wf % 128 == 0 else wf
    vmem = pl.BlockSpec(memory_space=pltpu.VMEM)
    hbm = pl.BlockSpec(memory_space=pltpu.HBM)
    sems = [pltpu.SemaphoreType.DMA((k,)) for k in (3, S, S, T, T, S, S, T // 2, T // 2, T // 2, T // 2)]
    return pl.pallas_call(
        functools.partial(body, rows, cols, side),
        out_shape=(jax.ShapeDtypeStruct((n, wf), f32), jax.ShapeDtypeStruct((n, wc), f32)),
        in_specs=[hbm] * 3,
        out_specs=(vmem, vmem),
        scratch_shapes=[
            pltpu.VMEM((S, height, wf), f32),
            pltpu.VMEM((T, height, wc), f32),
            pltpu.VMEM((4, n), f32),
            pltpu.VMEM((T, 3, wc, lanes), f32),
            pltpu.VMEM((T, 2 * n, wc), bf16),
            pltpu.VMEM((S, 2 * n, wf), bf16),
            pltpu.VMEM((2, wc, wf), bf16),
            pltpu.VMEM((2, wc, wf), bf16),
            pltpu.VMEM((S, n, wf), f32),
            pltpu.VMEM((S, n, wf), f32),
            pltpu.VMEM((T, n, wc), f32),
            pltpu.VMEM((T // 2, n, wc), f32),
            pltpu.VMEM((T // 2, n, wc), f32),
            *sems,
        ],
        compiler_params=pltpu.CompilerParams(
            collective_id=0, has_side_effects=True, vmem_limit_bytes=67_043_328
        ),
    )(fluid_data, center_data, poly_coef.T)


def solution(mesh):
    rows, cols = mesh.shape["row"], mesh.shape["col"]
    side = 2 if cols % 2 == 0 else 1
    placed = (P(None, ("row", "col")), P(None, ("col", "row")), P())
    return jax.shard_map(
        functools.partial(per_device, rows, cols, side),
        mesh=mesh,
        in_specs=placed,
        out_specs=(P(None, ("row", "col")), P(None, ("col", "row"))),
        check_vma=False,
    )
```

```python
import functools

import jax
import jax.numpy as jnp
from jax import lax
from jax.experimental import pallas as pl
from jax.experimental.pallas import tpu as pltpu
from jax.sharding import PartitionSpec as P

WAVES = 64
MESH = pl.DeviceIdType.MESH
TOP = 12.404427306735432
MID = 0.6418441597071612
LOW = 0.16126480593510223
X, Y, Z, CORES = 4, 4, 8, 2
GROUP = 4
PLANE = (
    ((1, 0), (3, 0), (0, 1), (0, 3))
    + ((2, 2), (2, 1), (2, 3), (1, 2))
    + ((3, 2), (1, 3), (3, 1), (3, 3))
    + ((2, 0), (0, 2), (1, 1), (0, 0))
)
OWN = len(PLANE) - 1
RING = (0, 1, 7, 2, 6, 3, 5, 4)
ORDER = tuple((c, p) for c in (0, 1) for p in range(4)) + tuple((c, p) for p in (3, 2, 1, 0) for c in (2, 3))
MERGED = (0, 1)


def dot(a, b, dims):
    return lax.dot_general(a, b, (dims, ((), ())), preferred_element_type=jnp.float32)


def split(x):
    high = x.astype(jnp.bfloat16)
    low = (x - high.astype(jnp.float32)).astype(jnp.bfloat16)
    return high, low


def body(fluid, center, poly, motion, loads, *scratch):
    fl, raw, ce, pv, cp, chl, fhl, fx, kh, kl, mo, mo_in, ld, ldp, pre, ld_in, ld_other = scratch[:17]
    own, fs, fr, cs, cr, os, orr, ms, mr, ps, pr, ls, lr, qs, qr = scratch[17:]
    row, col = lax.axis_index("row"), lax.axis_index("col")
    y, z, core = row // 4, ((row // 2) % 2) * 4 + col // 4, row % 2
    x = col % 4
    n, wf, wc = motion.shape[0], fluid.shape[1], center.shape[1]
    half = n // 2
    wide = 2 * wc
    step_rows = 32

    def at(dx, dy, dz, c):
        there = (z + dz) % Z
        return {
            "row": ((y + dy) % Y) * 4 + (there // 4) * 2 + c,
            "col": (there % 4) * 4 + (x + dx) % X,
        }

    def copy(src, dst, send, recv, where):
        return pltpu.make_async_remote_copy(
            src_ref=src, dst_ref=dst, send_sem=send, recv_sem=recv, device_id=where, device_id_type=MESH
        )

    sister = 1 - core

    def minus(s, c):
        dx, dy = PLANE[s]
        return at((X - dx) % X, (Y - dy) % Y, 0, c)

    def plus(s, c):
        dx, dy = PLANE[s]
        return at(dx, dy, 0, c)

    def send_fluid(m):
        return copy(fl.at[0], fl.at[m], fs.at[m], fr.at[m], at(0, 0, (Z - RING[m]) % Z, core))

    def send_center(s):
        return copy(ce.at[OWN, core], ce.at[s, core], cs.at[s], cr.at[s], minus(s, core))

    def send_across(s):
        return copy(ce.at[OWN, core], ce.at[s, core], os.at[s], orr.at[s], minus(s, sister))

    def hand_on(s):
        return copy(ce.at[s, core], ce.at[s, core], os.at[s], orr.at[s], at(0, 0, 0, sister))

    def from_other(s):
        return copy(ce.at[s, sister], ce.at[s, sister], os.at[s], orr.at[s], at(0, 0, 0, sister))

    def send_motion(m):
        return copy(mo.at[m], mo_in.at[m], ms.at[m], mr.at[m], at(0, 0, RING[m], core))

    def send_pre(s):
        return copy(ldp.at[s, sister], pre.at[s], ps.at[s], pr.at[s], at(0, 0, 0, sister))

    def send_loads(s):
        return copy(ldp.at[s, core], ld_in.at[s], ls.at[s], lr.at[s], plus(s, core))

    def send_loads_across(s):
        q = s - GROUP * len(MERGED)
        return copy(ldp.at[s, sister], ld_other.at[q], qs.at[q], qr.at[q], plus(s, sister))

    slots = [range(GROUP * c, GROUP * (c + 1)) for c in range(len(PLANE) // GROUP)]
    straight = slots[0]

    local = [
        pltpu.make_async_copy(center, raw, own.at[0]),
        pltpu.make_async_copy(fluid, fl.at[0], own.at[1]),
        pltpu.make_async_copy(poly, pv, own.at[2]),
    ]
    for c in local:
        c.start()
    barrier = pltpu.get_barrier_semaphore()
    greeted = [at(0, 0, RING[m], core) for m in range(1, Z)]
    greeted += [plus(s, core) for s in range(OWN)]
    greeted += [plus(s, sister) for s in straight]
    greeted += [minus(s, sister) for s in range(GROUP * len(MERGED), OWN + 1)]
    for where in greeted:
        pl.semaphore_signal(barrier, inc=1, device_id=where, device_id_type=MESH)
    for c in local:
        c.wait()
    coef = raw[3:, :] * TOP
    places = raw[0:8, :] * float(WAVES)
    ce[OWN, core, 0:half] = jnp.concatenate([coef[:half], coef[half:]], axis=1)
    ce[OWN, core, half:] = jnp.concatenate([places, places], axis=1)
    left = lax.broadcasted_iota(jnp.int32, (half, wide), 1) < wc
    left8 = lax.broadcasted_iota(jnp.int32, (8, wide), 1) < wc
    pl.semaphore_wait(barrier, len(greeted))
    send_fluid(1).start()
    for s in straight:
        send_center(s).start()
        send_across(s).start()
    for m in range(2, Z):
        send_fluid(m).start()
    send_across(OWN).start()
    for s in range(len(straight), OWN):
        send_center(s).start()

    def ready_center(c):
        for j, s in enumerate(slots[c]):
            a, b = ce[s, 0, 0:half], ce[s, 1, 0:half]
            upper = jnp.where(left, a, pltpu.roll(b, wc, 1))
            lower = jnp.where(left, pltpu.roll(a, wc, 1), b)
            high, low = split(jnp.concatenate([upper, lower], axis=0))
            part = pl.ds(j * wide, wide)
            chl[c, 0:n, part] = high
            chl[c, n:, part] = low
            spots = jnp.transpose(jnp.where(left8, ce[s, 0, half:], ce[s, 1, half:]))
            for a in range(3):
                cp[c, a, part, :] = jnp.broadcast_to(spots[:, a : a + 1], (wide, 128))

    def ready_fluid(p):
        for h in range(2):
            m = 2 * p + h
            part = pl.ds(h * wf, wf)
            high, low = split(fl[m, 3:, :] * TOP)
            fhl[p, 0:n, part] = high
            fhl[p, n:, part] = low
            fx[p, :, part] = fl[m, 0:8, :] * float(WAVES)

    def values(c, p, slot):
        for h in range(2):
            part = pl.ds(h * wf, wf)
            px, py, pz = (fx[p, a : a + 1, part] for a in range(3))
            for j in range(0, GROUP * wide, step_rows):
                rows = pl.ds(j, step_rows)
                dx, dy, dz = cp[c, 0, rows, :] - px, cp[c, 1, rows, :] - py, cp[c, 2, rows, :] - pz
                sq = dx * dx + dy * dy + dz * dz
                inv = lax.rsqrt(sq)
                turns = sq * inv
                f = turns - jnp.round(turns)
                size = jnp.abs(f)
                rest = 0.5 - size
                q = size * rest
                value = (f * rest * inv) * ((q + MID) * q + LOW)
                high, low = split(value)
                kh[slot, rows, part] = high
                kl[slot, rows, part] = low

    seen_c, seen_p = set(), set()

    def sums(c, p, slot):
        k_high, k_low = kh[slot], kl[slot]
        across = ((1,), (0,))
        both = dot(chl[c], k_high, across)
        out = both[:n] + both[n:] + dot(chl[c, 0:n], k_low, across)
        for h in range(2):
            piece = out[:, h * wf : (h + 1) * wf]
            mo[2 * p + h] = mo[2 * p + h] + piece if p in seen_p else piece
        back = ((1,), (1,))
        both = dot(fhl[p], k_high, back)
        out = both[:n] + both[n:] + dot(fhl[p, 0:n], k_low, back)
        ld[c] = ld[c] + out if c in seen_c else out
        seen_c.add(c)
        seen_p.add(p)

    def pack(c):
        for j, s in enumerate(slots[c]):
            part = pl.ds(j * wide, wide)
            upper, lower = ld[c, 0:half, part], ld[c, half:, part]
            ldp[s, 0] = jnp.where(left, upper, pltpu.roll(lower, wc, 1))
            ldp[s, 1] = jnp.where(left, pltpu.roll(upper, wc, 1), lower)

    def finished(k):
        c, p = ORDER[k]
        if all(o[1] != p for o in ORDER[k + 1 :]):
            for m in (2 * p + 1, 2 * p):
                if m:
                    send_motion(m).start()
        if all(o[0] != c for o in ORDER[k + 1 :]):
            pack(c)
            for s in slots[c]:
                if c in MERGED:
                    send_pre(s).start()
                else:
                    if s != OWN:
                        send_loads(s).start()
                    send_loads_across(s).start()
        if k and ORDER[k - 1][0] in MERGED and ORDER[k - 1][0] != c:
            for s in slots[ORDER[k - 1][0]]:
                send_pre(s).wait_recv()
                ldp[s, core] = ldp[s, core] + pre[s]
                send_loads(s).start()

    arrived_c, arrived_p = set(), set()
    handed = {1: 1, 2: 2, 3: 3}
    for k, (c, p) in enumerate(ORDER):
        if p not in arrived_p:
            for m in (2 * p, 2 * p + 1):
                if m:
                    send_fluid(m).wait_recv()
            ready_fluid(p)
            arrived_p.add(p)
        if k in handed:
            for s in slots[handed[k]]:
                if s != OWN:
                    send_center(s).wait_recv()
                    hand_on(s).start()
        if c not in arrived_c:
            for s in slots[c]:
                if s in straight:
                    send_center(s).wait_recv()
                from_other(s).wait_recv()
            ready_center(c)
            arrived_c.add(c)
        if k:
            sums(*ORDER[k - 1], (k - 1) % 2)
        values(c, p, k % 2)
        if k:
            finished(k - 1)
    last = len(ORDER) - 1
    sums(*ORDER[last], last % 2)
    finished(last)

    total = mo[0]
    affine = jnp.transpose(pv[...])
    for a in range(3):
        total = total + affine[:, a + 1 : a + 2] * fl[0, a : a + 1, :]
    total = total + affine[:, 0:1]
    for m in range(Z - 1, 0, -1):
        send_motion(m).wait_recv()
        total = total + mo_in[m]
    motion[...] = total
    total = ldp[OWN, core]
    for s in range(OWN):
        send_loads(s).wait_recv()
        total = total + ld_in[s]
    for s in range(GROUP * len(MERGED), OWN + 1):
        send_loads_across(s).wait_recv()
        total = total + ld_other[s - GROUP * len(MERGED)]
    loads[0:half, :] = total[:, :wc]
    loads[half:, :] = total[:, wc:]
    for m in range(1, Z):
        send_fluid(m).wait_send()
        send_motion(m).wait_send()
    for s in range(OWN + 1):
        if s != OWN:
            send_center(s).wait_send()
            send_loads(s).wait_send()
        (send_across(s) if s in straight or s == OWN else hand_on(s)).wait_send()
        if s < GROUP * len(MERGED):
            send_pre(s).wait_send()
        else:
            send_loads_across(s).wait_send()


def per_device(fluid_data, center_data, poly_coef):
    f32, bf16 = jnp.float32, jnp.bfloat16
    height, wf = fluid_data.shape
    wc = center_data.shape[1]
    n = height - 3
    slots, cols, rows = len(PLANE), len(PLANE) // GROUP, Z // 2
    deep, broad = GROUP * CORES * wc, 2 * wf
    merged = GROUP * len(MERGED)
    vmem = pl.BlockSpec(memory_space=pltpu.VMEM)
    hbm = pl.BlockSpec(memory_space=pltpu.HBM)
    counts = (3, Z, Z, slots, slots, slots, slots, Z, Z, merged, merged, slots, slots, slots - merged, slots - merged)
    return pl.pallas_call(
        body,
        out_shape=(jax.ShapeDtypeStruct((n, wf), f32), jax.ShapeDtypeStruct((n, wc), f32)),
        in_specs=[hbm] * 3,
        out_specs=(vmem, vmem),
        scratch_shapes=[
            pltpu.VMEM((Z, height, wf), f32),
            pltpu.VMEM((height, wc), f32),
            pltpu.VMEM((slots, CORES, n // 2 + 8, 2 * wc), f32),
            pltpu.VMEM((4, n), f32),
            pltpu.VMEM((cols, 3, deep, 128), f32),
            pltpu.VMEM((cols, 2 * n, deep), bf16),
            pltpu.VMEM((rows, 2 * n, broad), bf16),
            pltpu.VMEM((rows, 8, broad), f32),
            pltpu.VMEM((2, deep, broad), bf16),
            pltpu.VMEM((2, deep, broad), bf16),
            pltpu.VMEM((Z, n, wf), f32),
            pltpu.VMEM((Z, n, wf), f32),
            pltpu.VMEM((cols, n, deep), f32),
            pltpu.VMEM((slots, CORES, n // 2, 2 * wc), f32),
            pltpu.VMEM((merged, n // 2, 2 * wc), f32),
            pltpu.VMEM((slots, n // 2, 2 * wc), f32),
            pltpu.VMEM((slots - merged, n // 2, 2 * wc), f32),
            *[pltpu.SemaphoreType.DMA((k,)) for k in counts],
        ],
        compiler_params=pltpu.CompilerParams(
            collective_id=0, has_side_effects=True, vmem_limit_bytes=67_043_328
        ),
    )(fluid_data, center_data, poly_coef.T)


def solution(mesh):
    return jax.shard_map(
        per_device,
        mesh=mesh,
        in_specs=(P(None, ("row", "col")), P(None, ("col", "row")), P()),
        out_specs=(P(None, ("row", "col")), P(None, ("col", "row"))),
        check_vma=False,
    )
```

```python
import functools

import jax
import jax.numpy as jnp
from jax import lax
from jax.experimental import pallas as pl
from jax.experimental.pallas import tpu as pltpu
from jax.sharding import PartitionSpec as P

WAVES = 64
MESH = pl.DeviceIdType.MESH
TOP = 12.404427306735432
MID = 0.6418441597071612
LOW = 0.16126480593510223
X, Y, Z, CORES = 4, 4, 8, 2
GROUP = 4
PLANE = (
    ((1, 0), (3, 0), (0, 1), (0, 3))
    + ((1, 1), (1, 3), (3, 1), (3, 3))
    + ((2, 3), (1, 2), (3, 2), (2, 2))
    + ((2, 1), (2, 0), (0, 2), (0, 0))
)
OWN = len(PLANE) - 1
RING = (0, 1, 7, 2, 6, 3, 5, 4)
ORDER = (
    ((0, 0), (0, 1), (1, 0), (1, 1), (0, 2), (1, 2), (2, 2), (3, 2))
    + ((0, 3), (1, 3), (2, 3), (3, 3), (2, 1), (2, 0), (3, 1), (3, 0))
)
STRAIGHT = (0, 1)
HANDED = {3: 2, 4: 3}
READY = {0: 0, 2: 1, 5: 2, 6: 3}
MERGED = (0, 1, 2)


def dot(a, b, dims):
    return lax.dot_general(a, b, (dims, ((), ())), preferred_element_type=jnp.float32)


def split(x):
    high = x.astype(jnp.bfloat16)
    low = (x - high.astype(jnp.float32)).astype(jnp.bfloat16)
    return high, low


def body(fluid, center, poly, motion, loads, *scratch):
    fl, raw, ce, pv, cp, chl, fhl, fx, kh, kl, mo, mo_in, ld, ldp, pre, ld_in, ld_other = scratch[:17]
    own, fs, fr, cs, cr, os, orr, ms, mr, ps, pr, ls, lr, qs, qr = scratch[17:]
    row, col = lax.axis_index("row"), lax.axis_index("col")
    y, z, core = row // 4, ((row // 2) % 2) * 4 + col // 4, row % 2
    x = col % 4
    n, wf, wc = motion.shape[0], fluid.shape[1], center.shape[1]
    half = n // 2
    wide = 2 * wc
    step_rows = 32

    def at(dx, dy, dz, c):
        there = (z + dz) % Z
        return {
            "row": ((y + dy) % Y) * 4 + (there // 4) * 2 + c,
            "col": (there % 4) * 4 + (x + dx) % X,
        }

    def copy(src, dst, send, recv, where):
        return pltpu.make_async_remote_copy(
            src_ref=src, dst_ref=dst, send_sem=send, recv_sem=recv, device_id=where, device_id_type=MESH
        )

    sister = 1 - core

    def minus(s, c):
        dx, dy = PLANE[s]
        return at((X - dx) % X, (Y - dy) % Y, 0, c)

    def plus(s, c):
        dx, dy = PLANE[s]
        return at(dx, dy, 0, c)

    def send_fluid(m):
        return copy(fl.at[0], fl.at[m], fs.at[m], fr.at[m], at(0, 0, (Z - RING[m]) % Z, core))

    def send_center(s):
        return copy(ce.at[OWN, core], ce.at[s, core], cs.at[s], cr.at[s], minus(s, core))

    def send_across(s):
        return copy(ce.at[OWN, core], ce.at[s, core], os.at[s], orr.at[s], minus(s, sister))

    def hand_on(s):
        return copy(ce.at[s, core], ce.at[s, core], os.at[s], orr.at[s], at(0, 0, 0, sister))

    def from_other(s):
        return copy(ce.at[s, sister], ce.at[s, sister], os.at[s], orr.at[s], at(0, 0, 0, sister))

    def send_motion(m):
        return copy(mo.at[m], mo_in.at[m], ms.at[m], mr.at[m], at(0, 0, RING[m], core))

    def send_pre(s):
        return copy(ldp.at[s, sister], pre.at[s], ps.at[s], pr.at[s], at(0, 0, 0, sister))

    def send_loads(s):
        return copy(ldp.at[s, core], ld_in.at[s], ls.at[s], lr.at[s], plus(s, core))

    def send_loads_across(s):
        q = s - GROUP * len(MERGED)
        return copy(ldp.at[s, sister], ld_other.at[q], qs.at[q], qr.at[q], plus(s, sister))

    slots = [range(GROUP * c, GROUP * (c + 1)) for c in range(len(PLANE) // GROUP)]
    straight = [s for c in STRAIGHT for s in slots[c]]

    local = [
        pltpu.make_async_copy(center, raw, own.at[0]),
        pltpu.make_async_copy(fluid, fl.at[0], own.at[1]),
        pltpu.make_async_copy(poly, pv, own.at[2]),
    ]
    for c in local:
        c.start()
    barrier = pltpu.get_barrier_semaphore()
    greeted = [at(0, 0, RING[m], core) for m in range(1, Z)]
    greeted += [plus(s, core) for s in range(OWN)]
    greeted += [plus(s, sister) for s in straight]
    greeted += [minus(s, sister) for s in range(GROUP * len(MERGED), OWN + 1)]
    for where in greeted:
        pl.semaphore_signal(barrier, inc=1, device_id=where, device_id_type=MESH)
    for c in local:
        c.wait()
    coef = raw[3:, :] * TOP
    places = raw[0:8, :] * float(WAVES)
    ce[OWN, core, 0:half] = jnp.concatenate([coef[:half], coef[half:]], axis=1)
    ce[OWN, core, half:] = jnp.concatenate([places, places], axis=1)
    left = lax.broadcasted_iota(jnp.int32, (half, wide), 1) < wc
    left8 = lax.broadcasted_iota(jnp.int32, (8, wide), 1) < wc
    pl.semaphore_wait(barrier, len(greeted))
    send_fluid(1).start()
    for s in straight:
        send_center(s).start()
        send_across(s).start()
    for m in range(2, Z):
        send_fluid(m).start()
    send_across(OWN).start()
    for s in range(len(straight), OWN):
        send_center(s).start()

    def ready_center(c):
        for j, s in enumerate(slots[c]):
            a, b = ce[s, 0, 0:half], ce[s, 1, 0:half]
            upper = jnp.where(left, a, pltpu.roll(b, wc, 1))
            lower = jnp.where(left, pltpu.roll(a, wc, 1), b)
            high, low = split(jnp.concatenate([upper, lower], axis=0))
            part = pl.ds(j * wide, wide)
            chl[c, 0:n, part] = high
            chl[c, n:, part] = low
            spots = jnp.transpose(jnp.where(left8, ce[s, 0, half:], ce[s, 1, half:]))
            for a in range(3):
                cp[c, a, part, :] = jnp.broadcast_to(spots[:, a : a + 1], (wide, 128))

    def ready_fluid(p):
        for h in range(2):
            m = 2 * p + h
            part = pl.ds(h * wf, wf)
            high, low = split(fl[m, 3:, :] * TOP)
            fhl[p, 0:n, part] = high
            fhl[p, n:, part] = low
            fx[p, :, part] = fl[m, 0:8, :] * float(WAVES)

    def values(c, p, slot):
        for h in range(2):
            part = pl.ds(h * wf, wf)
            px, py, pz = (fx[p, a : a + 1, part] for a in range(3))
            for j in range(0, GROUP * wide, step_rows):
                rows = pl.ds(j, step_rows)
                dx, dy, dz = cp[c, 0, rows, :] - px, cp[c, 1, rows, :] - py, cp[c, 2, rows, :] - pz
                sq = dx * dx + dy * dy + dz * dz
                inv = lax.rsqrt(sq)
                turns = sq * inv
                f = turns - jnp.round(turns)
                size = jnp.abs(f)
                rest = 0.5 - size
                q = size * rest
                value = (f * rest * inv) * ((q + MID) * q + LOW)
                high, low = split(value)
                kh[slot, rows, part] = high
                kl[slot, rows, part] = low

    seen_c, seen_p = set(), set()

    def sums(c, p, slot):
        k_high, k_low = kh[slot], kl[slot]
        across = ((1,), (0,))
        both = dot(chl[c], k_high, across)
        out = both[:n] + both[n:] + dot(chl[c, 0:n], k_low, across)
        for h in range(2):
            piece = out[:, h * wf : (h + 1) * wf]
            mo[2 * p + h] = mo[2 * p + h] + piece if p in seen_p else piece
        back = ((1,), (1,))
        both = dot(fhl[p], k_high, back)
        out = both[:n] + both[n:] + dot(fhl[p, 0:n], k_low, back)
        ld[c] = ld[c] + out if c in seen_c else out
        seen_c.add(c)
        seen_p.add(p)

    def pack(c):
        for j, s in enumerate(slots[c]):
            part = pl.ds(j * wide, wide)
            upper, lower = ld[c, 0:half, part], ld[c, half:, part]
            ldp[s, 0] = jnp.where(left, upper, pltpu.roll(lower, wc, 1))
            ldp[s, 1] = jnp.where(left, pltpu.roll(upper, wc, 1), lower)

    merging = []

    def finished(k):
        c, p = ORDER[k]
        if all(o[1] != p for o in ORDER[k + 1 :]):
            for m in (2 * p + 1, 2 * p):
                if m:
                    send_motion(m).start()
        done = all(o[0] != c for o in ORDER[k + 1 :])
        if done:
            pack(c)
            for s in slots[c]:
                if c in MERGED:
                    send_pre(s).start()
                else:
                    if s != OWN:
                        send_loads(s).start()
                    send_loads_across(s).start()
        for s in merging:
            send_pre(s).wait_recv()
            ldp[s, core] = ldp[s, core] + pre[s]
            send_loads(s).start()
        merging[:] = slots[c] if done and c in MERGED else ()

    arrived_p = set()
    for k, (c, p) in enumerate(ORDER):
        if p not in arrived_p:
            for m in (2 * p, 2 * p + 1):
                if m:
                    send_fluid(m).wait_recv()
            ready_fluid(p)
            arrived_p.add(p)
        if k in HANDED:
            for s in slots[HANDED[k]]:
                if s != OWN:
                    send_center(s).wait_recv()
                    hand_on(s).start()
        if k in READY:
            for s in slots[READY[k]]:
                if s in straight:
                    send_center(s).wait_recv()
                from_other(s).wait_recv()
            ready_center(READY[k])
        if k:
            sums(*ORDER[k - 1], (k - 1) % 2)
        values(c, p, k % 2)
        if k:
            finished(k - 1)
    last = len(ORDER) - 1
    sums(*ORDER[last], last % 2)
    finished(last)

    total = mo[0]
    affine = jnp.transpose(pv[...])
    for a in range(3):
        total = total + affine[:, a + 1 : a + 2] * fl[0, a : a + 1, :]
    total = total + affine[:, 0:1]
    for m in range(Z - 1, 0, -1):
        send_motion(m).wait_recv()
        total = total + mo_in[m]
    motion[...] = total
    total = ldp[OWN, core]
    for s in range(OWN):
        send_loads(s).wait_recv()
        total = total + ld_in[s]
    for s in range(GROUP * len(MERGED), OWN + 1):
        send_loads_across(s).wait_recv()
        total = total + ld_other[s - GROUP * len(MERGED)]
    loads[0:half, :] = total[:, :wc]
    loads[half:, :] = total[:, wc:]
    for m in range(1, Z):
        send_fluid(m).wait_send()
        send_motion(m).wait_send()
    for s in range(OWN + 1):
        if s != OWN:
            send_center(s).wait_send()
            send_loads(s).wait_send()
        (send_across(s) if s in straight or s == OWN else hand_on(s)).wait_send()
        if s < GROUP * len(MERGED):
            send_pre(s).wait_send()
        else:
            send_loads_across(s).wait_send()


def per_device(fluid_data, center_data, poly_coef):
    f32, bf16 = jnp.float32, jnp.bfloat16
    height, wf = fluid_data.shape
    wc = center_data.shape[1]
    n = height - 3
    slots, cols, rows = len(PLANE), len(PLANE) // GROUP, Z // 2
    deep, broad = GROUP * CORES * wc, 2 * wf
    merged = GROUP * len(MERGED)
    vmem = pl.BlockSpec(memory_space=pltpu.VMEM)
    hbm = pl.BlockSpec(memory_space=pltpu.HBM)
    counts = (3, Z, Z, slots, slots, slots, slots, Z, Z, merged, merged, slots, slots, slots - merged, slots - merged)
    return pl.pallas_call(
        body,
        out_shape=(jax.ShapeDtypeStruct((n, wf), f32), jax.ShapeDtypeStruct((n, wc), f32)),
        in_specs=[hbm] * 3,
        out_specs=(vmem, vmem),
        scratch_shapes=[
            pltpu.VMEM((Z, height, wf), f32),
            pltpu.VMEM((height, wc), f32),
            pltpu.VMEM((slots, CORES, n // 2 + 8, 2 * wc), f32),
            pltpu.VMEM((4, n), f32),
            pltpu.VMEM((cols, 3, deep, 128), f32),
            pltpu.VMEM((cols, 2 * n, deep), bf16),
            pltpu.VMEM((rows, 2 * n, broad), bf16),
            pltpu.VMEM((rows, 8, broad), f32),
            pltpu.VMEM((2, deep, broad), bf16),
            pltpu.VMEM((2, deep, broad), bf16),
            pltpu.VMEM((Z, n, wf), f32),
            pltpu.VMEM((Z, n, wf), f32),
            pltpu.VMEM((cols, n, deep), f32),
            pltpu.VMEM((slots, CORES, n // 2, 2 * wc), f32),
            pltpu.VMEM((merged, n // 2, 2 * wc), f32),
            pltpu.VMEM((slots, n // 2, 2 * wc), f32),
            pltpu.VMEM((slots - merged, n // 2, 2 * wc), f32),
            *[pltpu.SemaphoreType.DMA((k,)) for k in counts],
        ],
        compiler_params=pltpu.CompilerParams(
            collective_id=0, has_side_effects=True, vmem_limit_bytes=67_043_328
        ),
    )(fluid_data, center_data, poly_coef.T)


def solution(mesh):
    return jax.shard_map(
        per_device,
        mesh=mesh,
        in_specs=(P(None, ("row", "col")), P(None, ("col", "row")), P()),
        out_specs=(P(None, ("row", "col")), P(None, ("col", "row"))),
        check_vma=False,
    )
```

```python
import functools

import jax
import jax.numpy as jnp
from jax import lax
from jax.experimental import pallas as pl
from jax.experimental.pallas import tpu as pltpu
from jax.sharding import PartitionSpec as P

WAVES = 64
MESH = pl.DeviceIdType.MESH
TOP = 12.404427306735432
MID = 0.6418441597071612
LOW = 0.16126480593510223
X, Y, Z, CORES = 4, 4, 8, 2
GROUP = 4
PLANE = (
    ((1, 0), (3, 0), (0, 1), (0, 3))
    + ((1, 1), (1, 3), (3, 1), (3, 3))
    + ((2, 3), (1, 2), (3, 2), (2, 2))
    + ((2, 1), (2, 0), (0, 2), (0, 0))
)
OWN = len(PLANE) - 1
RING = (0, 1, 7, 2, 6, 3, 5, 4)
ORDER = (
    ((0, 0), (0, 1), (1, 0), (1, 1), (0, 2), (1, 2), (2, 2), (3, 2))
    + ((0, 3), (1, 3), (2, 3), (3, 3), (2, 1), (2, 0), (3, 1), (3, 0))
)
STRAIGHT = (0, 1)
HANDED = {3: 2, 4: 3}
READY = {0: 0, 2: 1, 5: 2, 6: 3}
MERGED = (0, 1, 2)


def dot(a, b, dims):
    return lax.dot_general(a, b, (dims, ((), ())), preferred_element_type=jnp.float32)


def split(x):
    high = x.astype(jnp.bfloat16)
    low = (x - high.astype(jnp.float32)).astype(jnp.bfloat16)
    return high, low


def body(*refs):
    n, wf = refs[3].shape
    wc = refs[1].shape[1]
    deep, broad = GROUP * CORES * wc, 2 * wf
    pl.run_scoped(
        functools.partial(work, *refs),
        pltpu.VMEM((len(PLANE) // GROUP, 2 * n, deep), jnp.bfloat16),
        pltpu.VMEM((Z // 2, 2 * n, broad), jnp.bfloat16),
        pltpu.VMEM((2, deep, broad), jnp.bfloat16),
        pltpu.VMEM((2, deep, broad), jnp.bfloat16),
    )


def work(fluid, center, poly, motion, loads, *scratch):
    fl, raw, ce, pv, cp, fx, mo, mo_in, ld, ldp, pre, ld_in, ld_other = scratch[:13]
    own, fs, fr, cs, cr, os, orr, ms, mr, ps, pr, ls, lr, qs, qr = scratch[13:28]
    chl, fhl, kh, kl = scratch[28:]
    row, col = lax.axis_index("row"), lax.axis_index("col")
    y, z, core = row // 4, ((row // 2) % 2) * 4 + col // 4, row % 2
    x = col % 4
    n, wf, wc = motion.shape[0], fluid.shape[1], center.shape[1]
    half = n // 2
    wide = 2 * wc
    step_rows = 32

    def at(dx, dy, dz, c):
        there = (z + dz) % Z
        return {
            "row": ((y + dy) % Y) * 4 + (there // 4) * 2 + c,
            "col": (there % 4) * 4 + (x + dx) % X,
        }

    def copy(src, dst, send, recv, where):
        return pltpu.make_async_remote_copy(
            src_ref=src, dst_ref=dst, send_sem=send, recv_sem=recv, device_id=where, device_id_type=MESH
        )

    sister = 1 - core

    def minus(s, c):
        dx, dy = PLANE[s]
        return at((X - dx) % X, (Y - dy) % Y, 0, c)

    def plus(s, c):
        dx, dy = PLANE[s]
        return at(dx, dy, 0, c)

    def send_fluid(m):
        return copy(fl.at[0], fl.at[m], fs.at[m], fr.at[m], at(0, 0, (Z - RING[m]) % Z, core))

    def send_center(s):
        return copy(ce.at[OWN, core], ce.at[s, core], cs.at[s], cr.at[s], minus(s, core))

    def send_across(s):
        return copy(ce.at[OWN, core], ce.at[s, core], os.at[s], orr.at[s], minus(s, sister))

    def hand_on(s):
        return copy(ce.at[s, core], ce.at[s, core], os.at[s], orr.at[s], at(0, 0, 0, sister))

    def from_other(s):
        return copy(ce.at[s, sister], ce.at[s, sister], os.at[s], orr.at[s], at(0, 0, 0, sister))

    def send_motion(m):
        return copy(mo.at[m], mo_in.at[m], ms.at[m], mr.at[m], at(0, 0, RING[m], core))

    def send_pre(s):
        return copy(ldp.at[s, sister], pre.at[s], ps.at[s], pr.at[s], at(0, 0, 0, sister))

    def send_loads(s):
        return copy(ldp.at[s, core], ld_in.at[s], ls.at[s], lr.at[s], plus(s, core))

    def send_loads_across(s):
        q = s - GROUP * len(MERGED)
        return copy(ldp.at[s, sister], ld_other.at[q], qs.at[q], qr.at[q], plus(s, sister))

    slots = [range(GROUP * c, GROUP * (c + 1)) for c in range(len(PLANE) // GROUP)]
    straight = [s for c in STRAIGHT for s in slots[c]]

    local = [
        pltpu.make_async_copy(center, raw, own.at[0]),
        pltpu.make_async_copy(fluid, fl.at[0], own.at[1]),
        pltpu.make_async_copy(poly, pv, own.at[2]),
    ]
    for c in local:
        c.start()
    barrier = pltpu.get_barrier_semaphore()
    greeted = [at(0, 0, RING[m], core) for m in range(1, Z)]
    greeted += [plus(s, core) for s in range(OWN)]
    greeted += [plus(s, sister) for s in straight]
    greeted += [minus(s, sister) for s in range(GROUP * len(MERGED), OWN + 1)]
    for where in greeted:
        pl.semaphore_signal(barrier, inc=1, device_id=where, device_id_type=MESH)
    for c in local:
        c.wait()
    coef = raw[3:, :] * TOP
    places = raw[0:8, :] * float(WAVES)
    ce[OWN, core, 0:half] = jnp.concatenate([coef[:half], coef[half:]], axis=1)
    ce[OWN, core, half:] = jnp.concatenate([places, places], axis=1)
    left = lax.broadcasted_iota(jnp.int32, (half, wide), 1) < wc
    left8 = lax.broadcasted_iota(jnp.int32, (8, wide), 1) < wc
    pl.semaphore_wait(barrier, len(greeted))
    send_fluid(1).start()
    for s in straight:
        send_center(s).start()
        send_across(s).start()
    for m in range(2, Z):
        send_fluid(m).start()
    send_across(OWN).start()
    for s in range(len(straight), OWN):
        send_center(s).start()

    def ready_center(c):
        for j, s in enumerate(slots[c]):
            a, b = ce[s, 0, 0:half], ce[s, 1, 0:half]
            upper = jnp.where(left, a, pltpu.roll(b, wc, 1))
            lower = jnp.where(left, pltpu.roll(a, wc, 1), b)
            high, low = split(jnp.concatenate([upper, lower], axis=0))
            part = pl.ds(j * wide, wide)
            chl[c, 0:n, part] = high
            chl[c, n:, part] = low
            spots = jnp.transpose(jnp.where(left8, ce[s, 0, half:], ce[s, 1, half:]))
            for a in range(3):
                cp[c, a, part, :] = jnp.broadcast_to(spots[:, a : a + 1], (wide, 128))

    def ready_fluid(p):
        for h in range(2):
            m = 2 * p + h
            part = pl.ds(h * wf, wf)
            high, low = split(fl[m, 3:, :] * TOP)
            fhl[p, 0:n, part] = high
            fhl[p, n:, part] = low
            fx[p, :, part] = fl[m, 0:8, :] * float(WAVES)

    def values(c, p, slot):
        for h in range(2):
            part = pl.ds(h * wf, wf)
            px, py, pz = (fx[p, a : a + 1, part] for a in range(3))
            for j in range(0, GROUP * wide, step_rows):
                rows = pl.ds(j, step_rows)
                dx, dy, dz = cp[c, 0, rows, :] - px, cp[c, 1, rows, :] - py, cp[c, 2, rows, :] - pz
                sq = dx * dx + dy * dy + dz * dz
                inv = lax.rsqrt(sq)
                turns = sq * inv
                f = turns - jnp.round(turns)
                size = jnp.abs(f)
                rest = 0.5 - size
                q = size * rest
                value = (f * rest * inv) * ((q + MID) * q + LOW)
                high, low = split(value)
                kh[slot, rows, part] = high
                kl[slot, rows, part] = low

    seen_c, seen_p = set(), set()

    def sums(c, p, slot):
        k_high, k_low = kh[slot], kl[slot]
        across = ((1,), (0,))
        both = dot(chl[c], k_high, across)
        out = both[:n] + both[n:] + dot(chl[c, 0:n], k_low, across)
        for h in range(2):
            piece = out[:, h * wf : (h + 1) * wf]
            mo[2 * p + h] = mo[2 * p + h] + piece if p in seen_p else piece
        back = ((1,), (1,))
        both = dot(fhl[p], k_high, back)
        out = both[:n] + both[n:] + dot(fhl[p, 0:n], k_low, back)
        ld[c] = ld[c] + out if c in seen_c else out
        seen_c.add(c)
        seen_p.add(p)

    def pack(c):
        for j, s in enumerate(slots[c]):
            part = pl.ds(j * wide, wide)
            upper, lower = ld[c, 0:half, part], ld[c, half:, part]
            ldp[s, 0] = jnp.where(left, upper, pltpu.roll(lower, wc, 1))
            ldp[s, 1] = jnp.where(left, pltpu.roll(upper, wc, 1), lower)

    merging = []

    def finished(k):
        c, p = ORDER[k]
        if all(o[1] != p for o in ORDER[k + 1 :]):
            for m in (2 * p + 1, 2 * p):
                if m:
                    send_motion(m).start()
        done = all(o[0] != c for o in ORDER[k + 1 :])
        if done:
            pack(c)
            for s in slots[c]:
                if c in MERGED:
                    send_pre(s).start()
                else:
                    if s != OWN:
                        send_loads(s).start()
                    send_loads_across(s).start()
        for s in merging:
            send_pre(s).wait_recv()
            ldp[s, core] = ldp[s, core] + pre[s]
            send_loads(s).start()
        merging[:] = slots[c] if done and c in MERGED else ()

    arrived_p = set()
    for k, (c, p) in enumerate(ORDER):
        if p not in arrived_p:
            for m in (2 * p, 2 * p + 1):
                if m:
                    send_fluid(m).wait_recv()
            ready_fluid(p)
            arrived_p.add(p)
        if k in HANDED:
            for s in slots[HANDED[k]]:
                if s != OWN:
                    send_center(s).wait_recv()
                    hand_on(s).start()
        if k in READY:
            for s in slots[READY[k]]:
                if s in straight:
                    send_center(s).wait_recv()
                from_other(s).wait_recv()
            ready_center(READY[k])
        if k:
            sums(*ORDER[k - 1], (k - 1) % 2)
        values(c, p, k % 2)
        if k:
            finished(k - 1)
    last = len(ORDER) - 1
    sums(*ORDER[last], last % 2)
    finished(last)

    total = mo[0]
    affine = jnp.transpose(pv[...])
    for a in range(3):
        total = total + affine[:, a + 1 : a + 2] * fl[0, a : a + 1, :]
    total = total + affine[:, 0:1]
    for m in range(Z - 1, 0, -1):
        send_motion(m).wait_recv()
        total = total + mo_in[m]
    motion[...] = total
    total = ldp[OWN, core]
    for s in range(OWN):
        send_loads(s).wait_recv()
        total = total + ld_in[s]
    for s in range(GROUP * len(MERGED), OWN + 1):
        send_loads_across(s).wait_recv()
        total = total + ld_other[s - GROUP * len(MERGED)]
    loads[0:half, :] = total[:, :wc]
    loads[half:, :] = total[:, wc:]
    for m in range(1, Z):
        send_fluid(m).wait_send()
        send_motion(m).wait_send()
    for s in range(OWN + 1):
        if s != OWN:
            send_center(s).wait_send()
            send_loads(s).wait_send()
        (send_across(s) if s in straight or s == OWN else hand_on(s)).wait_send()
        if s < GROUP * len(MERGED):
            send_pre(s).wait_send()
        else:
            send_loads_across(s).wait_send()


def per_device(fluid_data, center_data, poly_coef):
    f32 = jnp.float32
    height, wf = fluid_data.shape
    wc = center_data.shape[1]
    n = height - 3
    slots, cols, rows = len(PLANE), len(PLANE) // GROUP, Z // 2
    deep, broad = GROUP * CORES * wc, 2 * wf
    merged = GROUP * len(MERGED)
    vmem = pl.BlockSpec(memory_space=pltpu.VMEM)
    hbm = pl.BlockSpec(memory_space=pltpu.HBM)
    counts = (3, Z, Z, slots, slots, slots, slots, Z, Z, merged, merged, slots, slots, slots - merged, slots - merged)
    return pl.pallas_call(
        body,
        out_shape=(jax.ShapeDtypeStruct((n, wf), f32), jax.ShapeDtypeStruct((n, wc), f32)),
        in_specs=[hbm] * 3,
        out_specs=(vmem, vmem),
        scratch_shapes=[
            pltpu.VMEM((Z, height, wf), f32),
            pltpu.VMEM((height, wc), f32),
            pltpu.VMEM((slots, CORES, n // 2 + 8, 2 * wc), f32),
            pltpu.VMEM((4, n), f32),
            pltpu.VMEM((cols, 3, deep, 128), f32),
            pltpu.VMEM((rows, 8, broad), f32),
            pltpu.VMEM((Z, n, wf), f32),
            pltpu.VMEM((Z, n, wf), f32),
            pltpu.VMEM((cols, n, deep), f32),
            pltpu.VMEM((slots, CORES, n // 2, 2 * wc), f32),
            pltpu.VMEM((merged, n // 2, 2 * wc), f32),
            pltpu.VMEM((slots, n // 2, 2 * wc), f32),
            pltpu.VMEM((slots - merged, n // 2, 2 * wc), f32),
            *[pltpu.SemaphoreType.DMA((k,)) for k in counts],
        ],
        compiler_params=pltpu.CompilerParams(
            collective_id=0, has_side_effects=True, vmem_limit_bytes=67_043_328
        ),
    )(fluid_data, center_data, poly_coef.T)


def solution(mesh):
    return jax.shard_map(
        per_device,
        mesh=mesh,
        in_specs=(P(None, ("row", "col")), P(None, ("col", "row")), P()),
        out_specs=(P(None, ("row", "col")), P(None, ("col", "row"))),
        check_vma=False,
    )
```

```python
import functools

import jax
import jax.numpy as jnp
from jax import lax
from jax.experimental import pallas as pl
from jax.experimental.pallas import tpu as pltpu
from jax.sharding import PartitionSpec as P

WAVES = 64
MESH = pl.DeviceIdType.MESH
TOP = 12.404427306735432
MID = 0.6418441597071612
LOW = 0.16126480593510223
X, Y, Z, CORES = 4, 4, 8, 2
GROUP = 4
PLANE = (
    ((1, 0), (3, 0), (0, 1), (0, 3))
    + ((1, 1), (1, 3), (3, 1), (3, 3))
    + ((2, 1), (2, 3), (1, 2), (2, 2))
    + ((3, 2), (2, 0), (0, 2), (0, 0))
)
OWN = len(PLANE) - 1
RING = (0, 1, 7, 2, 6, 3, 5, 4)
ORDER = (
    ((0, 0), (0, 1), (1, 0), (1, 1), (0, 2), (1, 2), (2, 2), (3, 2))
    + ((0, 3), (1, 3), (2, 3), (3, 3), (2, 1), (2, 0), (3, 1), (3, 0))
)
STRAIGHT = (0, 1)
HANDED = {3: 2, 4: 3}
READY = {0: 0, 2: 1, 5: 2, 6: 3}
MERGED = (0, 1, 2)
SENT = {8: (7,), 10: (8, 9), 12: (10, 11), 14: (12, 13), 15: (14,)}
SUMMED = {12: (0, 1), 15: (2,)}


def dot(a, b, dims):
    return lax.dot_general(a, b, (dims, ((), ())), preferred_element_type=jnp.float32)


def split(x):
    high = x.astype(jnp.bfloat16)
    low = (x - high.astype(jnp.float32)).astype(jnp.bfloat16)
    return high, low


def body(*refs):
    n, wf = refs[3].shape
    wc = refs[1].shape[1]
    deep, broad = GROUP * CORES * wc, 2 * wf
    pl.run_scoped(
        functools.partial(work, *refs),
        pltpu.VMEM((len(PLANE) // GROUP, 2 * n, deep), jnp.bfloat16),
        pltpu.VMEM((Z // 2, 2 * n, broad), jnp.bfloat16),
        pltpu.VMEM((2, deep, broad), jnp.bfloat16),
        pltpu.VMEM((2, deep, broad), jnp.bfloat16),
    )


def work(fluid, center, poly, motion, loads, *scratch):
    fl, raw, ce, pv, cp, fx, mo, mo_in, ld, ldp, pre, ld_in, ld_other = scratch[:13]
    own, fs, fr, cs, cr, os, orr, ms, mr, ps, pr, ls, lr, qs, qr = scratch[13:28]
    chl, fhl, kh, kl = scratch[28:]
    row, col = lax.axis_index("row"), lax.axis_index("col")
    y, z, core = row // 4, ((row // 2) % 2) * 4 + col // 4, row % 2
    x = col % 4
    n, wf, wc = motion.shape[0], fluid.shape[1], center.shape[1]
    half = n // 2
    wide = 2 * wc
    step_rows = 32

    def at(dx, dy, dz, c):
        there = (z + dz) % Z
        return {
            "row": ((y + dy) % Y) * 4 + (there // 4) * 2 + c,
            "col": (there % 4) * 4 + (x + dx) % X,
        }

    def copy(src, dst, send, recv, where):
        return pltpu.make_async_remote_copy(
            src_ref=src, dst_ref=dst, send_sem=send, recv_sem=recv, device_id=where, device_id_type=MESH
        )

    sister = 1 - core

    def minus(s, c):
        dx, dy = PLANE[s]
        return at((X - dx) % X, (Y - dy) % Y, 0, c)

    def plus(s, c):
        dx, dy = PLANE[s]
        return at(dx, dy, 0, c)

    def send_fluid(m):
        return copy(fl.at[0], fl.at[m], fs.at[m], fr.at[m], at(0, 0, (Z - RING[m]) % Z, core))

    def send_center(s):
        return copy(ce.at[OWN, core], ce.at[s, core], cs.at[s], cr.at[s], minus(s, core))

    def send_across(s):
        return copy(ce.at[OWN, core], ce.at[s, core], os.at[s], orr.at[s], minus(s, sister))

    def hand_on(s):
        return copy(ce.at[s, core], ce.at[s, core], os.at[s], orr.at[s], at(0, 0, 0, sister))

    def from_other(s):
        return copy(ce.at[s, sister], ce.at[s, sister], os.at[s], orr.at[s], at(0, 0, 0, sister))

    def send_motion(m):
        return copy(mo.at[m], mo_in.at[m], ms.at[m], mr.at[m], at(0, 0, RING[m], core))

    def send_pre(s):
        return copy(ldp.at[s, sister], pre.at[s], ps.at[s], pr.at[s], at(0, 0, 0, sister))

    def send_loads(s):
        return copy(ldp.at[s, core], ld_in.at[s], ls.at[s], lr.at[s], plus(s, core))

    def send_loads_across(s):
        q = s - GROUP * len(MERGED)
        return copy(ldp.at[s, sister], ld_other.at[q], qs.at[q], qr.at[q], plus(s, sister))

    slots = [range(GROUP * c, GROUP * (c + 1)) for c in range(len(PLANE) // GROUP)]
    straight = [s for c in STRAIGHT for s in slots[c]]

    local = [
        pltpu.make_async_copy(center, raw, own.at[0]),
        pltpu.make_async_copy(fluid, fl.at[0], own.at[1]),
        pltpu.make_async_copy(poly, pv, own.at[2]),
    ]
    for c in local:
        c.start()
    barrier = pltpu.get_barrier_semaphore()
    greeted = [at(0, 0, RING[m], core) for m in range(1, Z)]
    greeted += [plus(s, core) for s in range(OWN)]
    greeted += [plus(s, sister) for s in straight]
    greeted += [minus(s, sister) for s in range(GROUP * len(MERGED), OWN + 1)]
    for where in greeted:
        pl.semaphore_signal(barrier, inc=1, device_id=where, device_id_type=MESH)
    for c in local:
        c.wait()
    coef = raw[3:, :] * TOP
    places = raw[0:8, :] * float(WAVES)
    ce[OWN, core, 0:half] = jnp.concatenate([coef[:half], coef[half:]], axis=1)
    ce[OWN, core, half:] = jnp.concatenate([places, places], axis=1)
    left = lax.broadcasted_iota(jnp.int32, (half, wide), 1) < wc
    left8 = lax.broadcasted_iota(jnp.int32, (8, wide), 1) < wc
    pl.semaphore_wait(barrier, len(greeted))
    send_fluid(1).start()
    for s in straight:
        send_center(s).start()
        send_across(s).start()
    for m in range(2, Z):
        send_fluid(m).start()
    send_across(OWN).start()
    for s in range(len(straight), OWN):
        send_center(s).start()

    def ready_center(c):
        for j, s in enumerate(slots[c]):
            a, b = ce[s, 0, 0:half], ce[s, 1, 0:half]
            upper = jnp.where(left, a, pltpu.roll(b, wc, 1))
            lower = jnp.where(left, pltpu.roll(a, wc, 1), b)
            high, low = split(jnp.concatenate([upper, lower], axis=0))
            part = pl.ds(j * wide, wide)
            chl[c, 0:n, part] = high
            chl[c, n:, part] = low
            spots = jnp.transpose(jnp.where(left8, ce[s, 0, half:], ce[s, 1, half:]))
            for a in range(3):
                cp[c, a, part, :] = jnp.broadcast_to(spots[:, a : a + 1], (wide, 128))

    def ready_fluid(p):
        for h in range(2):
            m = 2 * p + h
            part = pl.ds(h * wf, wf)
            high, low = split(fl[m, 3:, :] * TOP)
            fhl[p, 0:n, part] = high
            fhl[p, n:, part] = low
            fx[p, :, part] = fl[m, 0:8, :] * float(WAVES)

    def values(c, p, slot):
        for h in range(2):
            part = pl.ds(h * wf, wf)
            px, py, pz = (fx[p, a : a + 1, part] for a in range(3))
            for j in range(0, GROUP * wide, step_rows):
                rows = pl.ds(j, step_rows)
                dx, dy, dz = cp[c, 0, rows, :] - px, cp[c, 1, rows, :] - py, cp[c, 2, rows, :] - pz
                sq = dx * dx + dy * dy + dz * dz
                inv = lax.rsqrt(sq)
                turns = sq * inv
                f = turns - jnp.round(turns)
                size = jnp.abs(f)
                rest = 0.5 - size
                q = size * rest
                value = (f * rest * inv) * ((q + MID) * q + LOW)
                high, low = split(value)
                kh[slot, rows, part] = high
                kl[slot, rows, part] = low

    seen_c, seen_p = set(), set()

    def sums(c, p, slot):
        k_high, k_low = kh[slot], kl[slot]
        across = ((1,), (0,))
        both = dot(chl[c], k_high, across)
        out = both[:n] + both[n:] + dot(chl[c, 0:n], k_low, across)
        for h in range(2):
            piece = out[:, h * wf : (h + 1) * wf]
            mo[2 * p + h] = mo[2 * p + h] + piece if p in seen_p else piece
        back = ((1,), (1,))
        both = dot(fhl[p], k_high, back)
        out = both[:n] + both[n:] + dot(fhl[p, 0:n], k_low, back)
        ld[c] = ld[c] + out if c in seen_c else out
        seen_c.add(c)
        seen_p.add(p)

    def pack(c):
        for j, s in enumerate(slots[c]):
            part = pl.ds(j * wide, wide)
            upper, lower = ld[c, 0:half, part], ld[c, half:, part]
            ldp[s, 0] = jnp.where(left, upper, pltpu.roll(lower, wc, 1))
            ldp[s, 1] = jnp.where(left, pltpu.roll(upper, wc, 1), lower)

    def finished(k):
        c, p = ORDER[k]
        if all(o[1] != p for o in ORDER[k + 1 :]):
            for m in (2 * p + 1, 2 * p):
                if m:
                    send_motion(m).start()
        if all(o[0] != c for o in ORDER[k + 1 :]):
            pack(c)
            for s in slots[c]:
                if c in MERGED:
                    send_pre(s).start()
                else:
                    if s != OWN:
                        send_loads(s).start()
                    send_loads_across(s).start()

    def merge(c):
        for s in slots[c]:
            send_pre(s).wait_recv()
            ldp[s, core] = ldp[s, core] + pre[s]
            send_loads(s).start()

    arrived_p = set()
    for k, (c, p) in enumerate(ORDER):
        if p not in arrived_p:
            for m in (2 * p, 2 * p + 1):
                if m:
                    send_fluid(m).wait_recv()
            ready_fluid(p)
            arrived_p.add(p)
        if k in HANDED:
            for s in slots[HANDED[k]]:
                if s != OWN:
                    send_center(s).wait_recv()
                    hand_on(s).start()
        if k in READY:
            for s in slots[READY[k]]:
                if s in straight:
                    send_center(s).wait_recv()
                from_other(s).wait_recv()
            ready_center(READY[k])
        if k:
            sums(*ORDER[k - 1], (k - 1) % 2)
        values(c, p, k % 2)
        for done in SENT.get(k, ()):
            finished(done)
        for done in SUMMED.get(k, ()):
            merge(done)
    last = len(ORDER) - 1
    sums(*ORDER[last], last % 2)
    finished(last)

    for m in range(1, Z):
        send_fluid(m).wait_send()
        if m > 3:
            send_motion(m).wait_send()
    for s in range(OWN + 1):
        if s != OWN:
            send_center(s).wait_send()
        (send_across(s) if s in straight or s == OWN else hand_on(s)).wait_send()
        if s not in slots[-1]:
            send_pre(s).wait_send()
            send_loads(s).wait_send()
    total = mo[0]
    affine = jnp.transpose(pv[...])
    for a in range(3):
        total = total + affine[:, a + 1 : a + 2] * fl[0, a : a + 1, :]
    total = total + affine[:, 0:1]
    for m in range(Z - 1, 0, -1):
        send_motion(m).wait_recv()
        total = total + mo_in[m]
    motion[...] = total
    total = ldp[OWN, core]
    for s in range(OWN):
        send_loads(s).wait_recv()
        total = total + ld_in[s]
    for s in range(GROUP * len(MERGED), OWN + 1):
        send_loads_across(s).wait_recv()
        total = total + ld_other[s - GROUP * len(MERGED)]
    loads[0:half, :] = total[:, :wc]
    loads[half:, :] = total[:, wc:]
    for m in (1, 2, 3):
        send_motion(m).wait_send()
    for s in slots[-1]:
        if s != OWN:
            send_loads(s).wait_send()
        send_loads_across(s).wait_send()


def per_device(fluid_data, center_data, poly_coef):
    f32 = jnp.float32
    height, wf = fluid_data.shape
    wc = center_data.shape[1]
    n = height - 3
    slots, cols, rows = len(PLANE), len(PLANE) // GROUP, Z // 2
    deep, broad = GROUP * CORES * wc, 2 * wf
    merged = GROUP * len(MERGED)
    vmem = pl.BlockSpec(memory_space=pltpu.VMEM)
    hbm = pl.BlockSpec(memory_space=pltpu.HBM)
    counts = (3, Z, Z, slots, slots, slots, slots, Z, Z, merged, merged, slots, slots, slots - merged, slots - merged)
    return pl.pallas_call(
        body,
        out_shape=(jax.ShapeDtypeStruct((n, wf), f32), jax.ShapeDtypeStruct((n, wc), f32)),
        in_specs=[hbm] * 3,
        out_specs=(vmem, vmem),
        scratch_shapes=[
            pltpu.VMEM((Z, height, wf), f32),
            pltpu.VMEM((height, wc), f32),
            pltpu.VMEM((slots, CORES, n // 2 + 8, 2 * wc), f32),
            pltpu.VMEM((4, n), f32),
            pltpu.VMEM((cols, 3, deep, 128), f32),
            pltpu.VMEM((rows, 8, broad), f32),
            pltpu.VMEM((Z, n, wf), f32),
            pltpu.VMEM((Z, n, wf), f32),
            pltpu.VMEM((cols, n, deep), f32),
            pltpu.VMEM((slots, CORES, n // 2, 2 * wc), f32),
            pltpu.VMEM((merged, n // 2, 2 * wc), f32),
            pltpu.VMEM((slots, n // 2, 2 * wc), f32),
            pltpu.VMEM((slots - merged, n // 2, 2 * wc), f32),
            *[pltpu.SemaphoreType.DMA((k,)) for k in counts],
        ],
        compiler_params=pltpu.CompilerParams(
            collective_id=0, has_side_effects=True, vmem_limit_bytes=67_043_328
        ),
    )(fluid_data, center_data, poly_coef.T)


def solution(mesh):
    return jax.shard_map(
        per_device,
        mesh=mesh,
        in_specs=(P(None, ("row", "col")), P(None, ("col", "row")), P()),
        out_specs=(P(None, ("row", "col")), P(None, ("col", "row"))),
        check_vma=False,
    )
```
